128 devices in a mesh: py: 8 (over z, x_hi), px: 4 (over y_hi, core), pz: 4 (over y_lo, x_lo).
Axes of the slice: x: 4 (x_hi: 2, x_lo: 2; x = x_hi * 2 + x_lo), y: 4 (y_hi: 2, y_lo: 2; y = y_hi * 2 + y_lo), z: 4, core: 2. Of those that a mesh axis runs over, the one named last changes fastest.
Arguments:
- initial_density: float32 [32, 256, 384, 128], P('py', 'px', 'pz'), may hold values from 0.2 to 1.8
- inverse_limit: float32 [32, 256, 384, 128], P('py', 'px', 'pz'), may hold values from 0.5 to 2
Outputs:
- temperature_end: float32 [32, 256, 384, 128], P('py', 'px', 'pz')
The draws below stay inside these ranges and needn't reach their ends.
All inputs are finite; a program needn't handle non-finite values.
Results may differ from the reference program's by a relative error of at most 0.00002.
Values sent between devices are 32-bit elements; how exact they have to be, the bound alone decides.
A program may use at most 384 MiB of HBM per device.

```python
import jax
import jax.numpy as jnp
from jax import lax

WIDTH_SECOND = 32
WIDTH_FIRST = 256
WIDTH_THIRD = 384
DEPTH_TOTAL = 128
STEPS = 3


def shard_levels(rng, shape, cuts, low, top_value):
    loudness = 1.0
    for position, shards_of in cuts:
        heights = jax.random.uniform(jax.random.fold_in(jax.random.fold_in(rng, 6), position), (shards_of,), jnp.float32, low / len(cuts), top_value / len(cuts))
        loudness = loudness * jnp.repeat(jnp.exp(heights), shape[position] // shards_of).reshape((-1,) + (1,) * (len(shape) - 1 - position))
    return loudness


def setup_inputs(seed: int = 0) -> dict:
    streams_of = jax.random.split(jax.random.key(seed), 3)
    return {
        "initial_density": jnp.clip(0.2 + 1.5999999 * jax.random.uniform(streams_of[0], (WIDTH_SECOND, WIDTH_FIRST, WIDTH_THIRD, DEPTH_TOTAL), jnp.float32) ** shard_levels(streams_of[0], (WIDTH_SECOND, WIDTH_FIRST, WIDTH_THIRD, DEPTH_TOTAL), ((0, 8), (1, 4), (2, 4)), -0.2, 0.2), 0.2, 1.8),
        "inverse_limit": jnp.clip(0.5 + 1.5 * jax.random.uniform(streams_of[1], (WIDTH_SECOND, WIDTH_FIRST, WIDTH_THIRD, DEPTH_TOTAL), jnp.float32) ** shard_levels(streams_of[1], (WIDTH_SECOND, WIDTH_FIRST, WIDTH_THIRD, DEPTH_TOTAL), ((0, 8), (1, 4), (2, 4)), -0.2, 0.2), 0.5, 2.0),
    }


def inner_cells(values, dims):
    for dim in dims:
        values = lax.slice_in_dim(values, 1, values.shape[dim] - 1, axis=dim)
    return values


def boundary_cells(values, dim, start, dims):
    remaining_parts = [other for other in dims if other != dim]
    values = inner_cells(values, remaining_parts)
    return lax.slice_in_dim(values, start, start + values.shape[dim] - 2, axis=dim)


def advance_population(haloed_population, inverse_limit):
    middle = inner_cells(haloed_population, (0, 1, 2))
    lower = [boundary_cells(haloed_population, dim, 0, (0, 1, 2)) for dim in (0, 1, 2)]
    upper = [boundary_cells(haloed_population, dim, 2, (0, 1, 2)) for dim in (0, 1, 2)]
    spread = lower[0] + upper[0] + lower[1] + upper[1] + lower[2] + upper[2] - 6.0 * middle
    return middle + 0.1 * spread + 0.2 * middle * (1.0 - middle * inverse_limit)


def reference(initial_density, inverse_limit):
    for step in range(STEPS):
        initial_density = advance_population(jnp.pad(initial_density, ((1, 1), (1, 1), (1, 1), (0, 0)), mode="constant"), inverse_limit)
    return initial_density
```

```python
import functools

import jax
import jax.numpy as jnp
from jax import lax
from jax.experimental import pallas as pl
from jax.experimental.pallas import tpu as pltpu
from jax.sharding import PartitionSpec as P

STEPS = 3
ROWS = 8
MESH = pl.DeviceIdType.MESH


def kernel(sizes, u_ref, inv_ref, out_ref, buf, inv, halo, pz_in, pz_out,
           load_sem, store_sem, py_send, py_recv, px_send, px_recv, pz_send, pz_recv):
    planes, rows, cols, _ = u_ref.shape
    chunks = rows // ROWS
    me = {axis: lax.axis_index(axis) for axis in sizes}

    def there(axis, side):
        return me[axis] > 0 if side == 0 else me[axis] < sizes[axis] - 1

    def peer(axis, side):
        return {axis: me[axis] + (1 if side else -1)}

    loads = [
        pltpu.make_async_copy(u_ref, buf.at[0, :, pl.ds(1, rows)], load_sem.at[0]),
        pltpu.make_async_copy(inv_ref, inv, load_sem.at[1]),
    ]
    for load in loads:
        load.start()

    barrier = pltpu.get_barrier_semaphore()
    for axis in sizes:
        for side in (0, 1):
            @pl.when(there(axis, side))
            def _():
                pl.semaphore_signal(barrier, inc=1, device_id=peer(axis, side), device_id_type=MESH)
    peers = sum(there(axis, side).astype(jnp.int32) for axis in sizes for side in (0, 1))
    pl.semaphore_wait(barrier, peers)

    def py_copy(step, side, k, with_side=None):
        face = 0 if side == 0 else planes - 1
        at = pl.multiple_of(k * ROWS, ROWS)
        if step == 0:
            src = u_ref.at[face, pl.ds(at, ROWS)]
        else:
            src = buf.at[step % 2, face, pl.ds(at + 1, ROWS)]
        return pltpu.make_async_remote_copy(
            src_ref=src, dst_ref=halo.at[step, 1 - side, pl.ds(at, ROWS)],
            send_sem=py_send.at[step, side, k], recv_sem=py_recv.at[step, 1 - side, k],
            device_id=peer("py", side if with_side is None else with_side), device_id_type=MESH)

    def px_copy(step, side, with_side=None):
        edge = 0 if side == 0 else rows - 1
        src = u_ref.at[:, edge] if step == 0 else buf.at[step % 2, :, edge + 1]
        return pltpu.make_async_remote_copy(
            src_ref=src, dst_ref=buf.at[step % 2, :, rows + 1 if side == 0 else 0],
            send_sem=px_send.at[step, side], recv_sem=px_recv.at[step, 1 - side],
            device_id=peer("px", side if with_side is None else with_side), device_id_type=MESH)

    def pz_copy(step, side, with_side=None):
        return pltpu.make_async_remote_copy(
            src_ref=pz_out.at[step, side], dst_ref=pz_in.at[step, 1 - side],
            send_sem=pz_send.at[step, side], recv_sem=pz_recv.at[step, 1 - side],
            device_id=peer("pz", side if with_side is None else with_side), device_id_type=MESH)

    def store(k):
        at = pl.multiple_of(k * ROWS, ROWS)
        return pltpu.make_async_copy(
            buf.at[STEPS % 2, :, pl.ds(at + 1, ROWS)], out_ref.at[:, pl.ds(at, ROWS)], store_sem.at[k])

    for side in (0, 1):
        @pl.when(there("px", side))
        def _():
            px_copy(0, side).start()

    def first_sends(k, carry):
        for side in (0, 1):
            @pl.when(there("py", side))
            def _():
                py_copy(0, side, k).start()
        return carry
    lax.fori_loop(0, chunks, first_sends, 0)

    for side in (0, 1):
        @pl.when(jnp.logical_not(there("py", side)))
        def _():
            def clear(r, carry):
                for step in range(STEPS):
                    halo[step, side, r] = jnp.zeros(halo.shape[3:], halo.dtype)
                return carry
            lax.fori_loop(0, rows, clear, 0)

        @pl.when(jnp.logical_not(there("px", side)))
        def _():
            for slot in (0, 1):
                for p in range(planes):
                    buf[slot, p, 0 if side == 0 else rows + 1] = jnp.zeros(buf.shape[3:], buf.dtype)

        @pl.when(jnp.logical_not(there("pz", side)))
        def _():
            for step in range(STEPS):
                for p in range(planes):
                    pz_in[step, side, p] = jnp.zeros(pz_in.shape[3:], pz_in.dtype)

    loads[0].wait()

    def pack(r, carry):
        for p in range(planes):
            pz_out[0, 0, p, pl.ds(r, 1)] = buf[0, p, r + 1, 0:1]
            pz_out[0, 1, p, pl.ds(r, 1)] = buf[0, p, r + 1, cols - 1:cols]
        return carry
    lax.fori_loop(0, rows, pack, 0)
    for side in (0, 1):
        @pl.when(there("pz", side))
        def _():
            pz_copy(0, side).start()
    loads[1].wait()

    for step in range(STEPS):
        now, later = step % 2, (step + 1) % 2
        for side in (0, 1):
            @pl.when(there("px", side))
            def _():
                px_copy(step, side).wait_send()
                px_copy(step, 1 - side, side).wait_recv()

            @pl.when(there("pz", side))
            def _():
                pz_copy(step, side).wait_send()
                pz_copy(step, 1 - side, side).wait_recv()

        def chunk(k, carry):
            for side in (0, 1):
                @pl.when(there("py", side))
                def _():
                    py_copy(step, 1 - side, k, side).wait_recv()
                    if step >= 1:
                        py_copy(step - 1, side, k).wait_send()

            def row(i, inner):
                r = k * ROWS + i
                for p in range(planes):
                    mid = buf[now, p, r + 1]
                    lower = halo[step, 0, r] if p == 0 else buf[now, p - 1, r + 1]
                    upper = halo[step, 1, r] if p == planes - 1 else buf[now, p + 1, r + 1]
                    left = jnp.concatenate([pz_in[step, 0, p, pl.ds(r, 1)], mid[:-1]], axis=0)
                    right = jnp.concatenate([mid[1:], pz_in[step, 1, p, pl.ds(r, 1)]], axis=0)
                    spread = lower + upper + buf[now, p, r] + buf[now, p, r + 2] + left + right - 6.0 * mid
                    new = mid + 0.1 * spread + 0.2 * mid * (1.0 - mid * inv[p, r])
                    buf[later, p, r + 1] = new
                    if step < STEPS - 1:
                        pz_out[step + 1, 0, p, pl.ds(r, 1)] = new[0:1]
                        pz_out[step + 1, 1, p, pl.ds(r, 1)] = new[cols - 1:cols]
                return inner
            lax.fori_loop(0, ROWS, row, 0)

            if step < STEPS - 1:
                for side in (0, 1):
                    @pl.when(there("py", side))
                    def _():
                        py_copy(step + 1, side, k).start()
            else:
                store(k).start()
            return carry
        lax.fori_loop(0, chunks, chunk, 0)

        if step < STEPS - 1:
            for side in (0, 1):
                @pl.when(there("px", side))
                def _():
                    px_copy(step + 1, side).start()

                @pl.when(there("pz", side))
                def _():
                    pz_copy(step + 1, side).start()

    def finish(k, carry):
        for side in (0, 1):
            @pl.when(there("py", side))
            def _():
                py_copy(STEPS - 1, side, k).wait_send()
        store(k).wait()
        return carry
    lax.fori_loop(0, chunks, finish, 0)


def local(sizes, u, inv):
    planes, rows, cols, levels = u.shape
    chunks = rows // ROWS
    dma = pltpu.SemaphoreType.DMA
    return pl.pallas_call(
        functools.partial(kernel, sizes),
        out_shape=jax.ShapeDtypeStruct(u.shape, u.dtype),
        in_specs=[pl.BlockSpec(memory_space=pl.ANY)] * 2,
        out_specs=pl.BlockSpec(memory_space=pl.ANY),
        scratch_shapes=[
            pltpu.VMEM((2, planes, rows + 2, cols, levels), u.dtype),
            pltpu.VMEM(u.shape, u.dtype),
            pltpu.VMEM((STEPS, 2, rows, cols, levels), u.dtype),
            pltpu.VMEM((STEPS, 2, planes, rows, levels), u.dtype),
            pltpu.VMEM((STEPS, 2, planes, rows, levels), u.dtype),
            dma((2,)),
            dma((chunks,)),
            dma((STEPS, 2, chunks)),
            dma((STEPS, 2, chunks)),
            dma((STEPS, 2)),
            dma((STEPS, 2)),
            dma((STEPS, 2)),
            dma((STEPS, 2)),
        ],
        compiler_params=pltpu.CompilerParams(
            collective_id=0, has_side_effects=True, vmem_limit_bytes=67043328),
    )(u, inv)


def solution(mesh):
    spec = P("py", "px", "pz", None)
    sizes = {axis: mesh.shape[axis] for axis in ("py", "px", "pz")}
    return jax.shard_map(functools.partial(local, sizes), mesh=mesh, in_specs=(spec, spec),
                         out_specs=spec, check_vma=False)
```

```python
import functools

import jax
import jax.numpy as jnp
from jax import lax
from jax.experimental import pallas as pl
from jax.experimental.pallas import tpu as pltpu
from jax.sharding import PartitionSpec as P

STEPS = 3
ROWS = 8
MESH = pl.DeviceIdType.MESH


def share(n, k):
    return k % 4 < n


def kernel(sizes, u_ref, inv_ref, out_ref, transit, buf, inv, halo, pz_in, pz_out,
           load_sem, store_sem, py_send, py_recv, px_send, px_recv, pz_send, pz_recv,
           via_send, via_recv):
    planes, rows, cols, _ = u_ref.shape
    chunks = rows // ROWS
    ahead = chunks // 2
    me = {axis: lax.axis_index(axis) for axis in sizes}
    last = sizes["py"] - 1
    parity = [me["py"] % 2 == 0, me["py"] % 2 == 1]
    mine = ((last + 1 - me["py"]) // 2, (me["py"] + 1) // 2)
    others = ((last - 1 - me["py"]) // 2, (me["py"] - 1) // 2)

    def there(axis, side):
        return me[axis] > 0 if side == 0 else me[axis] < sizes[axis] - 1

    def peer(axis, side):
        return {axis: me[axis] + (1 if side else -1)}

    loads = [
        pltpu.make_async_copy(u_ref, buf.at[0, :, pl.ds(1, rows)], load_sem.at[0]),
        pltpu.make_async_copy(inv_ref, inv, load_sem.at[1]),
    ]
    for load in loads:
        load.start()

    barrier = pltpu.get_barrier_semaphore()
    peers = jnp.int32(0)
    for axis in sizes:
        for side in (0, 1):
            peers += there(axis, side).astype(jnp.int32)

            @pl.when(there(axis, side))
            def _():
                pl.semaphore_signal(barrier, inc=1, device_id=peer(axis, side), device_id_type=MESH)
    for far, exists in ((me["py"] - 2, me["py"] > 1), (me["py"] + 2, me["py"] < last - 1)):
        peers += exists.astype(jnp.int32)

        @pl.when(exists)
        def _():
            pl.semaphore_signal(barrier, inc=1, device_id={"py": far}, device_id_type=MESH)
    pl.semaphore_wait(barrier, peers)

    def source(step, side, k):
        face = 0 if side == 0 else planes - 1
        at = pl.multiple_of(k * ROWS, ROWS)
        if step == 0:
            return u_ref.at[face, pl.ds(at, ROWS)]
        return buf.at[step % 2, face, pl.ds(at + 1, ROWS)]

    def py_copy(step, side, k, device=None):
        at = pl.multiple_of(k * ROWS, ROWS)
        return pltpu.make_async_remote_copy(
            src_ref=source(step, side, k), dst_ref=halo.at[step, 1 - side, pl.ds(at, ROWS)],
            send_sem=py_send.at[step, side, k], recv_sem=py_recv.at[step, 1 - side, k],
            device_id=peer("py", side) if device is None else device, device_id_type=MESH)

    def via_copy(step, q, k):
        return pltpu.make_async_remote_copy(
            src_ref=source(step, q, k), dst_ref=transit.at[step, k],
            send_sem=py_send.at[step, q, k], recv_sem=via_recv.at[step, k],
            device_id={"py": me["py"] + (2 if q else -2)}, device_id_type=MESH)

    def on_copy(step, q, k):
        at = pl.multiple_of(k * ROWS, ROWS)
        return pltpu.make_async_remote_copy(
            src_ref=transit.at[step, k], dst_ref=halo.at[step, 1 - q, pl.ds(at, ROWS)],
            send_sem=via_send.at[step, k], recv_sem=py_recv.at[step, 1 - q, k],
            device_id=peer("py", 1 - q), device_id_type=MESH)

    def px_copy(step, side, with_side=None):
        edge = 0 if side == 0 else rows - 1
        src = u_ref.at[:, edge] if step == 0 else buf.at[step % 2, :, edge + 1]
        return pltpu.make_async_remote_copy(
            src_ref=src, dst_ref=buf.at[step % 2, :, rows + 1 if side == 0 else 0],
            send_sem=px_send.at[step, side], recv_sem=px_recv.at[step, 1 - side],
            device_id=peer("px", side if with_side is None else with_side), device_id_type=MESH)

    def pz_copy(step, side, with_side=None):
        return pltpu.make_async_remote_copy(
            src_ref=pz_out.at[step, side], dst_ref=pz_in.at[step, 1 - side],
            send_sem=pz_send.at[step, side], recv_sem=pz_recv.at[step, 1 - side],
            device_id=peer("pz", side if with_side is None else with_side), device_id_type=MESH)

    def store(k):
        at = pl.multiple_of(k * ROWS, ROWS)
        return pltpu.make_async_copy(
            buf.at[STEPS % 2, :, pl.ds(at + 1, ROWS)], out_ref.at[:, pl.ds(at, ROWS)], store_sem.at[k])

    def goes_via(q, k):
        return jnp.logical_and(jnp.logical_and(parity[q], there("py", q)), share(mine[q], k))

    def held(q, k):
        return jnp.logical_and(parity[q], share(others[q], k))

    def send_early(step, k):
        for q in (0, 1):
            @pl.when(goes_via(q, k))
            def _():
                via_copy(step, q, k).start()

    def send(step, k):
        for q in (0, 1):
            @pl.when(jnp.logical_and(there("py", q), jnp.logical_not(goes_via(q, k))))
            def _():
                py_copy(step, q, k).start()

            @pl.when(held(q, k))
            def _():
                via_copy(step, q, k).wait_recv()
                on_copy(step, q, k).start()

    def sent(step, k):
        for q in (0, 1):
            @pl.when(there("py", q))
            def _():
                py_copy(step, q, k).wait_send()

            @pl.when(held(q, k))
            def _():
                on_copy(step, q, k).wait_send()

    for side in (0, 1):
        @pl.when(there("px", side))
        def _():
            px_copy(0, side).start()

    def loop(count, body, start=0):
        def step(k, carry):
            body(k)
            return carry
        lax.fori_loop(start, count, step, 0)

    loop(chunks, lambda k: send_early(0, k))
    loop(ahead, lambda k: send(0, k))

    for side in (0, 1):
        @pl.when(jnp.logical_not(there("px", side)))
        def _():
            for slot in (0, 1):
                for p in range(planes):
                    buf[slot, p, 0 if side == 0 else rows + 1] = jnp.zeros(buf.shape[3:], buf.dtype)

        @pl.when(jnp.logical_not(there("pz", side)))
        def _():
            for step in range(STEPS):
                for p in range(planes):
                    pz_in[step, side, p] = jnp.zeros(pz_in.shape[3:], pz_in.dtype)

    loads[0].wait()

    def pack(r):
        for p in range(planes):
            pz_out[0, 0, p, pl.ds(r, 1)] = buf[0, p, r + 1, 0:1]
            pz_out[0, 1, p, pl.ds(r, 1)] = buf[0, p, r + 1, cols - 1:cols]
    loop(rows, pack)
    for side in (0, 1):
        @pl.when(there("pz", side))
        def _():
            pz_copy(0, side).start()
    loads[1].wait()

    inside = [there("py", side) for side in (0, 1)]
    for step in range(STEPS):
        now, later = step % 2, (step + 1) % 2
        for side in (0, 1):
            @pl.when(there("px", side))
            def _():
                px_copy(step, side).wait_send()
                px_copy(step, 1 - side, side).wait_recv()

            @pl.when(there("pz", side))
            def _():
                pz_copy(step, side).wait_send()
                pz_copy(step, 1 - side, side).wait_recv()

        def chunk(k, half):
            if half == 0:
                send(step, k + ahead)
            for side in (0, 1):
                @pl.when(there("py", side))
                def _():
                    py_copy(step, 1 - side, k, peer("py", side)).wait_recv()
            if step >= 1:
                sent(step - 1, k)

            def row(i):
                r = k * ROWS + i
                for p in range(planes):
                    mid = buf[now, p, r + 1]
                    lower = jnp.where(inside[0], halo[step, 0, r], 0.0) if p == 0 else buf[now, p - 1, r + 1]
                    upper = jnp.where(inside[1], halo[step, 1, r], 0.0) if p == planes - 1 else buf[now, p + 1, r + 1]
                    left = jnp.concatenate([pz_in[step, 0, p, pl.ds(r, 1)], mid[:-1]], axis=0)
                    right = jnp.concatenate([mid[1:], pz_in[step, 1, p, pl.ds(r, 1)]], axis=0)
                    spread = lower + upper + buf[now, p, r] + buf[now, p, r + 2] + left + right - 6.0 * mid
                    new = mid + 0.1 * spread + 0.2 * mid * (1.0 - mid * inv[p, r])
                    buf[later, p, r + 1] = new
                    if step < STEPS - 1:
                        pz_out[step + 1, 0, p, pl.ds(r, 1)] = new[0:1]
                        pz_out[step + 1, 1, p, pl.ds(r, 1)] = new[cols - 1:cols]
            loop(ROWS, row)

            if step < STEPS - 1:
                send_early(step + 1, k)
                if half == 1:
                    send(step + 1, k - ahead)
            else:
                store(k).start()

        loop(ahead, lambda k: chunk(k, 0))
        loop(chunks, lambda k: chunk(k, 1), ahead)

        if step < STEPS - 1:
            for side in (0, 1):
                @pl.when(there("px", side))
                def _():
                    px_copy(step + 1, side).start()

                @pl.when(there("pz", side))
                def _():
                    pz_copy(step + 1, side).start()

    def finish(k):
        sent(STEPS - 1, k)
        store(k).wait()
    loop(chunks, finish)


def local(sizes, u, inv):
    planes, rows, cols, levels = u.shape
    chunks = rows // ROWS
    dma = pltpu.SemaphoreType.DMA
    return pl.pallas_call(
        functools.partial(kernel, sizes),
        out_shape=(jax.ShapeDtypeStruct(u.shape, u.dtype),
                   jax.ShapeDtypeStruct((STEPS, chunks, ROWS, cols, levels), u.dtype)),
        in_specs=[pl.BlockSpec(memory_space=pl.ANY)] * 2,
        out_specs=(pl.BlockSpec(memory_space=pl.ANY),) * 2,
        scratch_shapes=[
            pltpu.VMEM((2, planes, rows + 2, cols, levels), u.dtype),
            pltpu.VMEM(u.shape, u.dtype),
            pltpu.VMEM((STEPS, 2, rows, cols, levels), u.dtype),
            pltpu.VMEM((STEPS, 2, planes, rows, levels), u.dtype),
            pltpu.VMEM((STEPS, 2, planes, rows, levels), u.dtype),
            dma((2,)),
            dma((chunks,)),
            dma((STEPS, 2, chunks)),
            dma((STEPS, 2, chunks)),
            dma((STEPS, 2)),
            dma((STEPS, 2)),
            dma((STEPS, 2)),
            dma((STEPS, 2)),
            dma((STEPS, chunks)),
            dma((STEPS, chunks)),
        ],
        compiler_params=pltpu.CompilerParams(
            collective_id=0, has_side_effects=True, vmem_limit_bytes=67043328),
    )(u, inv)[0]


def solution(mesh):
    spec = P("py", "px", "pz", None)
    sizes = {axis: mesh.shape[axis] for axis in ("py", "px", "pz")}
    return jax.shard_map(functools.partial(local, sizes), mesh=mesh, in_specs=(spec, spec),
                         out_specs=spec, check_vma=False)
```

```python
import functools

import jax
import jax.numpy as jnp
from jax import lax
from jax.experimental import pallas as pl
from jax.experimental.pallas import tpu as pltpu
from jax.sharding import PartitionSpec as P

STEPS = 3
ROWS = 4
AHEAD = 8
EARLY = 2
MESH = pl.DeviceIdType.MESH


def share(n, k):
    return k % 4 < n


def half(k):
    return k % 2 == 1


def kernel(sizes, u_ref, inv_ref, out_ref, transit, buf0, inv, halo, pz_in, pz_out,
           load_sem, py_send, py_recv, px_send, px_recv, pz_send, pz_recv,
           via_send, via_recv, pz_transit, pz_via_send, pz_via_recv):
    planes, rows, cols, _ = u_ref.shape
    chunks = rows // ROWS
    bufs = (buf0, out_ref)
    me = {axis: lax.axis_index(axis) for axis in sizes}
    last = sizes["py"] - 1
    parity = [me["py"] % 2 == 0, me["py"] % 2 == 1]
    mine = ((last + 1 - me["py"]) // 2, (me["py"] + 1) // 2)
    others = ((last - 1 - me["py"]) // 2, (me["py"] - 1) // 2)

    def there(axis, side):
        return me[axis] > 0 if side == 0 else me[axis] < sizes[axis] - 1

    def peer(axis, side):
        return {axis: me[axis] + (1 if side else -1)}

    def loop(count, body, start=0):
        def step(k, carry):
            body(k)
            return carry
        lax.fori_loop(start, count, step, 0)

    loads = [
        pltpu.make_async_copy(u_ref, buf0.at[:, pl.ds(1, rows)], load_sem.at[0]),
        pltpu.make_async_copy(inv_ref, inv, load_sem.at[1]),
    ]
    for load in loads:
        load.start()

    barrier = pltpu.get_barrier_semaphore()
    peers = jnp.int32(0)
    for axis in sizes:
        for side in (0, 1):
            peers += there(axis, side).astype(jnp.int32)

            @pl.when(there(axis, side))
            def _():
                pl.semaphore_signal(barrier, inc=1, device_id=peer(axis, side), device_id_type=MESH)
    for axis in ("py", "pz"):
        for far, exists in ((me[axis] - 2, me[axis] > 1), (me[axis] + 2, me[axis] < sizes[axis] - 2)):
            peers += exists.astype(jnp.int32)

            @pl.when(exists)
            def _():
                pl.semaphore_signal(barrier, inc=1, device_id={axis: far}, device_id_type=MESH)
    pl.semaphore_wait(barrier, peers)

    def source(step, side, k):
        face = 0 if side == 0 else planes - 1
        at = pl.multiple_of(k * ROWS, ROWS)
        if step == 0:
            return u_ref.at[face, pl.ds(at, ROWS)]
        return bufs[step % 2].at[face, pl.ds(at + 1, ROWS)]

    def py_copy(step, side, k, device=None):
        at = pl.multiple_of(k * ROWS, ROWS)
        return pltpu.make_async_remote_copy(
            src_ref=source(step, side, k), dst_ref=halo.at[step, 1 - side, pl.ds(at, ROWS)],
            send_sem=py_send.at[step, side, k], recv_sem=py_recv.at[step, 1 - side, k],
            device_id=peer("py", side) if device is None else device, device_id_type=MESH)

    def via_copy(step, q, k):
        return pltpu.make_async_remote_copy(
            src_ref=source(step, q, k), dst_ref=transit.at[step, k],
            send_sem=py_send.at[step, q, k], recv_sem=via_recv.at[step, k],
            device_id={"py": me["py"] + (2 if q else -2)}, device_id_type=MESH)

    def on_copy(step, q, k):
        at = pl.multiple_of(k * ROWS, ROWS)
        return pltpu.make_async_remote_copy(
            src_ref=transit.at[step, k], dst_ref=halo.at[step, 1 - q, pl.ds(at, ROWS)],
            send_sem=via_send.at[step, k], recv_sem=py_recv.at[step, 1 - q, k],
            device_id=peer("py", 1 - q), device_id_type=MESH)

    def px_copy(step, side, device=None):
        edge = 0 if side == 0 else rows - 1
        src = u_ref.at[:, edge] if step == 0 else bufs[step % 2].at[:, edge + 1]
        return pltpu.make_async_remote_copy(
            src_ref=src, dst_ref=bufs[step % 2].at[:, rows + 1 if side == 0 else 0],
            send_sem=px_send.at[step, side], recv_sem=px_recv.at[step, 1 - side],
            device_id=peer("px", side) if device is None else device, device_id_type=MESH)

    def pz_copy(step, side, k, device=None):
        return pltpu.make_async_remote_copy(
            src_ref=pz_out.at[step, side, k], dst_ref=pz_in.at[step, 1 - side, k],
            send_sem=pz_send.at[step, side, k], recv_sem=pz_recv.at[step, 1 - side, k],
            device_id=peer("pz", side) if device is None else device, device_id_type=MESH)

    def pz_via_copy(step, q, k):
        return pltpu.make_async_remote_copy(
            src_ref=pz_out.at[step, q, k], dst_ref=pz_transit.at[step, k],
            send_sem=pz_send.at[step, q, k], recv_sem=pz_via_recv.at[step, k],
            device_id={"pz": me["pz"] + (2 if q else -2)}, device_id_type=MESH)

    def pz_on_copy(step, q, k):
        return pltpu.make_async_remote_copy(
            src_ref=pz_transit.at[step, k], dst_ref=pz_in.at[step, 1 - q, k],
            send_sem=pz_via_send.at[step, k], recv_sem=pz_recv.at[step, 1 - q, k],
            device_id=peer("pz", 1 - q), device_id_type=MESH)

    pz_sender = (me["pz"] == 2, me["pz"] == 1)
    pz_helper = (me["pz"] == 0, me["pz"] == 3)

    def px_start(step, side):
        @pl.when(there("px", side))
        def _():
            px_copy(step, side).start()

    def px_arrived(step, side):
        @pl.when(there("px", side))
        def _():
            px_copy(step, 1 - side, peer("px", side)).wait_recv()

    def px_sent(step, side):
        @pl.when(there("px", side))
        def _():
            px_copy(step, side).wait_send()

    def pz_start(step, k):
        for side in (0, 1):
            via = jnp.logical_and(pz_sender[side], half(k))

            @pl.when(jnp.logical_and(there("pz", side), jnp.logical_not(via)))
            def _():
                pz_copy(step, side, k).start()

            @pl.when(via)
            def _():
                pz_via_copy(step, side, k).start()

    def pz_pass(step, k):
        for q in (0, 1):
            @pl.when(jnp.logical_and(pz_helper[q], half(k)))
            def _():
                pz_via_copy(step, q, k).wait_recv()
                pz_on_copy(step, q, k).start()

    def goes_via(q, k):
        return jnp.logical_and(jnp.logical_and(parity[q], there("py", q)), share(mine[q], k))

    def held(q, k):
        return jnp.logical_and(parity[q], share(others[q], k))

    def send_early(step, k):
        for q in (0, 1):
            @pl.when(goes_via(q, k))
            def _():
                via_copy(step, q, k).start()

    def send(step, k):
        for q in (0, 1):
            @pl.when(jnp.logical_and(there("py", q), jnp.logical_not(goes_via(q, k))))
            def _():
                py_copy(step, q, k).start()

            @pl.when(held(q, k))
            def _():
                via_copy(step, q, k).wait_recv()
                on_copy(step, q, k).start()

    def sent(step, k):
        for q in (0, 1):
            @pl.when(there("py", q))
            def _():
                py_copy(step, q, k).wait_send()

            @pl.when(there("pz", q))
            def _():
                pz_copy(step, q, k).wait_send()

            @pl.when(jnp.logical_and(pz_helper[q], half(k)))
            def _():
                pz_on_copy(step, q, k).wait_send()

            @pl.when(held(q, k))
            def _():
                on_copy(step, q, k).wait_send()

    loop(chunks, lambda k: send_early(0, k))
    loop(EARLY, lambda k: send(0, k))
    for side in (0, 1):
        px_start(0, side)

    for side in (0, 1):
        @pl.when(jnp.logical_not(there("px", side)))
        def _():
            for slot in bufs:
                for p in range(planes):
                    slot[p, 0 if side == 0 else rows + 1] = jnp.zeros(slot.shape[2:], slot.dtype)

        @pl.when(jnp.logical_not(there("pz", side)))
        def _():
            for step in range(STEPS):
                for k in range(chunks):
                    pz_in[step, side, k] = jnp.zeros(pz_in.shape[3:], pz_in.dtype)

    loads[0].wait()

    def pack(k):
        for i in range(ROWS):
            for p in range(planes):
                pz_out[0, 0, k, p * ROWS + i:p * ROWS + i + 1] = buf0[p, k * ROWS + i + 1, 0:1]
                pz_out[0, 1, k, p * ROWS + i:p * ROWS + i + 1] = buf0[p, k * ROWS + i + 1, cols - 1:cols]
        pz_start(0, k)
    loop(chunks, pack)
    loop(AHEAD, lambda k: pz_pass(0, k))
    loop(AHEAD, lambda k: send(0, k), EARLY)
    loads[1].wait()

    inside = [there("py", side) for side in (0, 1)]

    for step in range(STEPS):
        now, later = bufs[step % 2], bufs[(step + 1) % 2]

        def update(k, which):
            def row(i):
                r = k * ROWS + i
                for p in which:
                    mid = now[p, r + 1]
                    lower = jnp.where(inside[0], halo[step, 0, r], 0.0) if p == 0 else now[p - 1, r + 1]
                    upper = jnp.where(inside[1], halo[step, 1, r], 0.0) if p == planes - 1 else now[p + 1, r + 1]
                    left = jnp.concatenate([pz_in[step, 0, k, pl.ds(p * ROWS + i, 1)], mid[:-1]], axis=0)
                    right = jnp.concatenate([mid[1:], pz_in[step, 1, k, pl.ds(p * ROWS + i, 1)]], axis=0)
                    spread = lower + upper + now[p, r] + now[p, r + 2] + left + right - 6.0 * mid
                    new = mid + 0.1 * spread + 0.2 * mid * (1.0 - mid * inv[p, r])
                    later[p, r + 1] = new
                    if step < STEPS - 1:
                        pz_out[step + 1, 0, k, pl.ds(p * ROWS + i, 1)] = new[0:1]
                        pz_out[step + 1, 1, k, pl.ds(p * ROWS + i, 1)] = new[cols - 1:cols]
            loop(ROWS, row)

        def chunk(k):
            for side in (0, 1):
                @pl.when(there("pz", side))
                def _():
                    pz_copy(step, 1 - side, k, peer("pz", side)).wait_recv()
            if step >= 1:
                sent(step - 1, k)
            update(k, range(1, planes - 1))
            for side in (0, 1):
                @pl.when(there("py", side))
                def _():
                    py_copy(step, 1 - side, k, peer("py", side)).wait_recv()
            update(k, (0, planes - 1))
            if step < STEPS - 1:
                send_early(step + 1, k)
                pz_start(step + 1, k)

        def first(k):
            pz_pass(step, k + AHEAD)
            send(step, k + AHEAD)
            chunk(k)

        def second(k):
            chunk(k)
            if step < STEPS - 1:
                pz_pass(step + 1, k - (chunks - AHEAD))
                send(step + 1, k - (chunks - AHEAD))

        px_arrived(step, 0)
        loop(chunks - AHEAD, first)
        if step < STEPS - 1:
            px_start(step + 1, 0)
        px_arrived(step, 1)
        for side in (0, 1):
            px_sent(step, side)
        loop(chunks, second, chunks - AHEAD)
        if step < STEPS - 1:
            px_start(step + 1, 1)

    loop(chunks, lambda k: sent(STEPS - 1, k))


def drain(held_ref, out_ref, sem):
    rows = out_ref.shape[1]
    copies = [
        pltpu.make_async_copy(held_ref.at[p, pl.ds(1, rows)], out_ref.at[p], sem.at[p])
        for p in range(out_ref.shape[0])
    ]
    for copy in copies:
        copy.start()
    for copy in copies:
        copy.wait()


def local(sizes, u, inv):
    planes, rows, cols, levels = u.shape
    chunks = rows // ROWS
    dma = pltpu.SemaphoreType.DMA
    held, _ = pl.pallas_call(
        functools.partial(kernel, sizes),
        out_shape=(pltpu.VMEM((planes, rows + 2, cols, levels), u.dtype),
                   jax.ShapeDtypeStruct((STEPS, chunks, ROWS, cols, levels), u.dtype)),
        in_specs=[pl.BlockSpec(memory_space=pl.ANY)] * 2,
        out_specs=(pl.BlockSpec(memory_space=pltpu.VMEM), pl.BlockSpec(memory_space=pl.ANY)),
        scratch_shapes=[
            pltpu.VMEM((planes, rows + 2, cols, levels), u.dtype),
            pltpu.VMEM(u.shape, u.dtype),
            pltpu.VMEM((STEPS, 2, rows, cols, levels), u.dtype),
            pltpu.VMEM((STEPS, 2, chunks, planes * ROWS, levels), u.dtype),
            pltpu.VMEM((STEPS, 2, chunks, planes * ROWS, levels), u.dtype),
            dma((2,)),
            dma((STEPS, 2, chunks)),
            dma((STEPS, 2, chunks)),
            dma((STEPS, 2)),
            dma((STEPS, 2)),
            dma((STEPS, 2, chunks)),
            dma((STEPS, 2, chunks)),
            dma((STEPS, chunks)),
            dma((STEPS, chunks)),
            pltpu.VMEM((STEPS, chunks, planes * ROWS, levels), u.dtype),
            dma((STEPS, chunks)),
            dma((STEPS, chunks)),
        ],
        compiler_params=pltpu.CompilerParams(
            collective_id=0, has_side_effects=True, vmem_limit_bytes=48 * 2**20),
    )(u, inv)
    return pl.pallas_call(
        drain,
        out_shape=jax.ShapeDtypeStruct(u.shape, u.dtype),
        in_specs=[pl.BlockSpec(memory_space=pltpu.VMEM)],
        out_specs=pl.BlockSpec(memory_space=pl.ANY),
        scratch_shapes=[dma((planes,))],
        compiler_params=pltpu.CompilerParams(vmem_limit_bytes=2**20),
    )(held)


def solution(mesh):
    spec = P("py", "px", "pz", None)
    sizes = {axis: mesh.shape[axis] for axis in ("py", "px", "pz")}
    return jax.shard_map(functools.partial(local, sizes), mesh=mesh, in_specs=(spec, spec),
                         out_specs=spec, check_vma=False)
```

```python
import functools

import jax
import jax.numpy as jnp
from jax import lax
from jax.experimental import pallas as pl
from jax.experimental.pallas import tpu as pltpu
from jax.sharding import PartitionSpec as P

STEPS = 3
ROWS = 8
AHEAD = 4
EARLY = 2
MESH = pl.DeviceIdType.MESH


def share(n, k):
    return k % 4 >= 4 - n


def half(k):
    return k % 2 == 1


def kernel(sizes, u_ref, inv_ref, out_ref, transit, buf0, inv, halo, pz_in, pz_out,
           load_sem, py_send, py_recv, px_send, px_recv, pz_send, pz_recv,
           via_send, via_recv, pz_transit, pz_via_send, pz_via_recv):
    planes, rows, cols, _ = u_ref.shape
    chunks = rows // ROWS
    bufs = (buf0, out_ref)
    me = {axis: lax.axis_index(axis) for axis in sizes}
    last = sizes["py"] - 1
    parity = [me["py"] % 2 == 0, me["py"] % 2 == 1]
    mine = ((last + 1 - me["py"]) // 2, (me["py"] + 1) // 2)
    others = ((last - 1 - me["py"]) // 2, (me["py"] - 1) // 2)

    def there(axis, side):
        return me[axis] > 0 if side == 0 else me[axis] < sizes[axis] - 1

    def peer(axis, side):
        return {axis: me[axis] + (1 if side else -1)}

    def loop(count, body, start=0):
        def step(k, carry):
            body(k)
            return carry
        lax.fori_loop(start, count, step, 0)

    loads = [
        pltpu.make_async_copy(u_ref, buf0.at[:, pl.ds(1, rows)], load_sem.at[0]),
        pltpu.make_async_copy(inv_ref, inv, load_sem.at[1]),
    ]
    for load in loads:
        load.start()

    barrier = pltpu.get_barrier_semaphore()
    peers = jnp.int32(0)
    for axis in sizes:
        for side in (0, 1):
            peers += there(axis, side).astype(jnp.int32)

            @pl.when(there(axis, side))
            def _():
                pl.semaphore_signal(barrier, inc=1, device_id=peer(axis, side), device_id_type=MESH)
    for axis in ("py", "pz"):
        for far, exists in ((me[axis] - 2, me[axis] > 1), (me[axis] + 2, me[axis] < sizes[axis] - 2)):
            peers += exists.astype(jnp.int32)

            @pl.when(exists)
            def _():
                pl.semaphore_signal(barrier, inc=1, device_id={axis: far}, device_id_type=MESH)
    pl.semaphore_wait(barrier, peers)

    def source(step, side, k):
        face = 0 if side == 0 else planes - 1
        at = pl.multiple_of(k * ROWS, ROWS)
        if step == 0:
            return u_ref.at[face, pl.ds(at, ROWS)]
        return bufs[step % 2].at[face, pl.ds(at + 1, ROWS)]

    def py_copy(step, side, k, device=None):
        at = pl.multiple_of(k * ROWS, ROWS)
        return pltpu.make_async_remote_copy(
            src_ref=source(step, side, k), dst_ref=halo.at[step, 1 - side, pl.ds(at, ROWS)],
            send_sem=py_send.at[step, side, k], recv_sem=py_recv.at[step, 1 - side, k],
            device_id=peer("py", side) if device is None else device, device_id_type=MESH)

    def via_copy(step, q, k):
        return pltpu.make_async_remote_copy(
            src_ref=source(step, q, k), dst_ref=transit.at[step, k],
            send_sem=py_send.at[step, q, k], recv_sem=via_recv.at[step, k],
            device_id={"py": me["py"] + (2 if q else -2)}, device_id_type=MESH)

    def on_copy(step, q, k):
        at = pl.multiple_of(k * ROWS, ROWS)
        return pltpu.make_async_remote_copy(
            src_ref=transit.at[step, k], dst_ref=halo.at[step, 1 - q, pl.ds(at, ROWS)],
            send_sem=via_send.at[step, k], recv_sem=py_recv.at[step, 1 - q, k],
            device_id=peer("py", 1 - q), device_id_type=MESH)

    def px_copy(step, side, device=None):
        edge = 0 if side == 0 else rows - 1
        src = u_ref.at[:, edge] if step == 0 else bufs[step % 2].at[:, edge + 1]
        return pltpu.make_async_remote_copy(
            src_ref=src, dst_ref=bufs[step % 2].at[:, rows + 1 if side == 0 else 0],
            send_sem=px_send.at[step, side], recv_sem=px_recv.at[step, 1 - side],
            device_id=peer("px", side) if device is None else device, device_id_type=MESH)

    def pz_copy(step, side, k, device=None):
        return pltpu.make_async_remote_copy(
            src_ref=pz_out.at[step, side, k], dst_ref=pz_in.at[step, 1 - side, k],
            send_sem=pz_send.at[step, side, k], recv_sem=pz_recv.at[step, 1 - side, k],
            device_id=peer("pz", side) if device is None else device, device_id_type=MESH)

    def pz_via_copy(step, q, k):
        return pltpu.make_async_remote_copy(
            src_ref=pz_out.at[step, q, k], dst_ref=pz_transit.at[step, k],
            send_sem=pz_send.at[step, q, k], recv_sem=pz_via_recv.at[step, k],
            device_id={"pz": me["pz"] + (2 if q else -2)}, device_id_type=MESH)

    def pz_on_copy(step, q, k):
        return pltpu.make_async_remote_copy(
            src_ref=pz_transit.at[step, k], dst_ref=pz_in.at[step, 1 - q, k],
            send_sem=pz_via_send.at[step, k], recv_sem=pz_recv.at[step, 1 - q, k],
            device_id=peer("pz", 1 - q), device_id_type=MESH)

    pz_sender = (me["pz"] == 2, me["pz"] == 1)
    pz_helper = (me["pz"] == 0, me["pz"] == 3)

    def px_start(step, side):
        @pl.when(there("px", side))
        def _():
            px_copy(step, side).start()

    def px_arrived(step, side):
        @pl.when(there("px", side))
        def _():
            px_copy(step, 1 - side, peer("px", side)).wait_recv()

    def px_sent(step, side):
        @pl.when(there("px", side))
        def _():
            px_copy(step, side).wait_send()

    def pz_start(step, k):
        for side in (0, 1):
            via = jnp.logical_and(pz_sender[side], half(k))

            @pl.when(jnp.logical_and(there("pz", side), jnp.logical_not(via)))
            def _():
                pz_copy(step, side, k).start()

            @pl.when(via)
            def _():
                pz_via_copy(step, side, k).start()

    def pz_pass(step, k):
        for q in (0, 1):
            @pl.when(jnp.logical_and(pz_helper[q], half(k)))
            def _():
                pz_via_copy(step, q, k).wait_recv()
                pz_on_copy(step, q, k).start()

    def goes_via(q, k):
        return jnp.logical_and(jnp.logical_and(parity[q], there("py", q)), share(mine[q], k))

    def held(q, k):
        return jnp.logical_and(parity[q], share(others[q], k))

    def send_early(step, k):
        for q in (0, 1):
            @pl.when(goes_via(q, k))
            def _():
                via_copy(step, q, k).start()

    def send(step, k):
        for q in (0, 1):
            @pl.when(jnp.logical_and(there("py", q), jnp.logical_not(goes_via(q, k))))
            def _():
                py_copy(step, q, k).start()

            @pl.when(held(q, k))
            def _():
                via_copy(step, q, k).wait_recv()
                on_copy(step, q, k).start()

    def sent(step, k):
        for q in (0, 1):
            @pl.when(there("py", q))
            def _():
                py_copy(step, q, k).wait_send()

            @pl.when(there("pz", q))
            def _():
                pz_copy(step, q, k).wait_send()

            @pl.when(jnp.logical_and(pz_helper[q], half(k)))
            def _():
                pz_on_copy(step, q, k).wait_send()

            @pl.when(held(q, k))
            def _():
                on_copy(step, q, k).wait_send()

    loop(chunks, lambda k: send_early(0, k))
    loop(EARLY, lambda k: send(0, k))
    for side in (0, 1):
        px_start(0, side)

    for side in (0, 1):
        @pl.when(jnp.logical_not(there("px", side)))
        def _():
            for slot in bufs:
                for p in range(planes):
                    slot[p, 0 if side == 0 else rows + 1] = jnp.zeros(slot.shape[2:], slot.dtype)

        @pl.when(jnp.logical_not(there("pz", side)))
        def _():
            for step in range(STEPS):
                for k in range(chunks):
                    pz_in[step, side, k] = jnp.zeros(pz_in.shape[3:], pz_in.dtype)

    loads[0].wait()

    def pack(k):
        for i in range(ROWS):
            for p in range(planes):
                pz_out[0, 0, k, p * ROWS + i:p * ROWS + i + 1] = buf0[p, k * ROWS + i + 1, 0:1]
                pz_out[0, 1, k, p * ROWS + i:p * ROWS + i + 1] = buf0[p, k * ROWS + i + 1, cols - 1:cols]
        pz_start(0, k)
    loop(chunks, pack)
    loop(AHEAD, lambda k: pz_pass(0, k))
    loop(AHEAD, lambda k: send(0, k), EARLY)
    loads[1].wait()

    inside = [there("py", side) for side in (0, 1)]

    for step in range(STEPS):
        now, later = bufs[step % 2], bufs[(step + 1) % 2]

        def update(k, which):
            def row(i):
                r = k * ROWS + i
                for p in which:
                    mid = now[p, r + 1]
                    lower = jnp.where(inside[0], halo[step, 0, r], 0.0) if p == 0 else now[p - 1, r + 1]
                    upper = jnp.where(inside[1], halo[step, 1, r], 0.0) if p == planes - 1 else now[p + 1, r + 1]
                    left = jnp.concatenate([pz_in[step, 0, k, pl.ds(p * ROWS + i, 1)], mid[:-1]], axis=0)
                    right = jnp.concatenate([mid[1:], pz_in[step, 1, k, pl.ds(p * ROWS + i, 1)]], axis=0)
                    spread = lower + upper + now[p, r] + now[p, r + 2] + left + right - 6.0 * mid
                    new = mid + 0.1 * spread + 0.2 * mid * (1.0 - mid * inv[p, r])
                    later[p, r + 1] = new
                    if step < STEPS - 1:
                        pz_out[step + 1, 0, k, pl.ds(p * ROWS + i, 1)] = new[0:1]
                        pz_out[step + 1, 1, k, pl.ds(p * ROWS + i, 1)] = new[cols - 1:cols]
            loop(ROWS, row)

        def chunk(k):
            for side in (0, 1):
                @pl.when(there("pz", side))
                def _():
                    pz_copy(step, 1 - side, k, peer("pz", side)).wait_recv()
            if step >= 1:
                sent(step - 1, k)
            update(k, range(1, planes - 1))
            for side in (0, 1):
                @pl.when(there("py", side))
                def _():
                    py_copy(step, 1 - side, k, peer("py", side)).wait_recv()
            update(k, (0, planes - 1))
            if step < STEPS - 1:
                send_early(step + 1, k)
                pz_start(step + 1, k)

        def first(k):
            pz_pass(step, k + AHEAD)
            send(step, k + AHEAD)
            chunk(k)

        def second(k):
            chunk(k)
            if step < STEPS - 1:
                pz_pass(step + 1, k - (chunks - AHEAD))
                send(step + 1, k - (chunks - AHEAD))

        px_arrived(step, 0)
        loop(chunks - AHEAD, first)
        if step < STEPS - 1:
            px_start(step + 1, 0)
        px_arrived(step, 1)
        for side in (0, 1):
            px_sent(step, side)
        loop(chunks, second, chunks - AHEAD)
        if step < STEPS - 1:
            px_start(step + 1, 1)

    loop(chunks, lambda k: sent(STEPS - 1, k))


def drain(held_ref, out_ref, sem):
    rows = out_ref.shape[1]
    copies = [
        pltpu.make_async_copy(held_ref.at[p, pl.ds(1, rows)], out_ref.at[p], sem.at[p])
        for p in range(out_ref.shape[0])
    ]
    for copy in copies:
        copy.start()
    for copy in copies:
        copy.wait()


def local(sizes, u, inv):
    planes, rows, cols, levels = u.shape
    chunks = rows // ROWS
    dma = pltpu.SemaphoreType.DMA
    held, _ = pl.pallas_call(
        functools.partial(kernel, sizes),
        out_shape=(pltpu.VMEM((planes, rows + 2, cols, levels), u.dtype),
                   jax.ShapeDtypeStruct((STEPS, chunks, ROWS, cols, levels), u.dtype)),
        in_specs=[pl.BlockSpec(memory_space=pl.ANY)] * 2,
        out_specs=(pl.BlockSpec(memory_space=pltpu.VMEM), pl.BlockSpec(memory_space=pl.ANY)),
        scratch_shapes=[
            pltpu.VMEM((planes, rows + 2, cols, levels), u.dtype),
            pltpu.VMEM(u.shape, u.dtype),
            pltpu.VMEM((STEPS, 2, rows, cols, levels), u.dtype),
            pltpu.VMEM((STEPS, 2, chunks, planes * ROWS, levels), u.dtype),
            pltpu.VMEM((STEPS, 2, chunks, planes * ROWS, levels), u.dtype),
            dma((2,)),
            dma((STEPS, 2, chunks)),
            dma((STEPS, 2, chunks)),
            dma((STEPS, 2)),
            dma((STEPS, 2)),
            dma((STEPS, 2, chunks)),
            dma((STEPS, 2, chunks)),
            dma((STEPS, chunks)),
            dma((STEPS, chunks)),
            pltpu.VMEM((STEPS, chunks, planes * ROWS, levels), u.dtype),
            dma((STEPS, chunks)),
            dma((STEPS, chunks)),
        ],
        compiler_params=pltpu.CompilerParams(
            collective_id=0, has_side_effects=True, vmem_limit_bytes=48 * 2**20),
    )(u, inv)
    return pl.pallas_call(
        drain,
        out_shape=jax.ShapeDtypeStruct(u.shape, u.dtype),
        in_specs=[pl.BlockSpec(memory_space=pltpu.VMEM)],
        out_specs=pl.BlockSpec(memory_space=pl.ANY),
        scratch_shapes=[dma((planes,))],
        compiler_params=pltpu.CompilerParams(vmem_limit_bytes=2**20),
    )(held)


def solution(mesh):
    spec = P("py", "px", "pz", None)
    sizes = {axis: mesh.shape[axis] for axis in ("py", "px", "pz")}
    return jax.shard_map(functools.partial(local, sizes), mesh=mesh, in_specs=(spec, spec),
                         out_specs=spec, check_vma=False)
```

```python
import functools

import jax
import jax.numpy as jnp
from jax import lax
from jax.experimental import pallas as pl
from jax.experimental.pallas import tpu as pltpu
from jax.sharding import PartitionSpec as P

STEPS = 3
ROWS = 16
AHEAD = 2
EARLY = 1
MESH = pl.DeviceIdType.MESH


def share(n, k):
    return k % 4 >= 4 - n


def half(k):
    return k % 2 == 1


def kernel(sizes, u_ref, inv_ref, out_ref, transit, buf0, inv, halo, pz_in, pz_out,
           load_sem, py_send, py_recv, px_send, px_recv, pz_send, pz_recv,
           via_send, via_recv, pz_transit, pz_via_send, pz_via_recv):
    planes, rows, cols, _ = u_ref.shape
    chunks = rows // ROWS
    bufs = (buf0, out_ref)
    me = {axis: lax.axis_index(axis) for axis in sizes}
    last = sizes["py"] - 1
    parity = [me["py"] % 2 == 0, me["py"] % 2 == 1]
    mine = ((last + 1 - me["py"]) // 2, (me["py"] + 1) // 2)
    others = ((last - 1 - me["py"]) // 2, (me["py"] - 1) // 2)

    def there(axis, side):
        return me[axis] > 0 if side == 0 else me[axis] < sizes[axis] - 1

    def peer(axis, side):
        return {axis: me[axis] + (1 if side else -1)}

    def loop(count, body, start=0):
        def step(k, carry):
            body(k)
            return carry
        lax.fori_loop(start, count, step, 0)

    loads = [
        pltpu.make_async_copy(u_ref, buf0.at[:, pl.ds(1, rows)], load_sem.at[0]),
        pltpu.make_async_copy(inv_ref, inv, load_sem.at[1]),
    ]
    for load in loads:
        load.start()

    barrier = pltpu.get_barrier_semaphore()
    peers = jnp.int32(0)
    for axis in sizes:
        for side in (0, 1):
            peers += there(axis, side).astype(jnp.int32)

            @pl.when(there(axis, side))
            def _():
                pl.semaphore_signal(barrier, inc=1, device_id=peer(axis, side), device_id_type=MESH)
    for axis in ("py", "pz"):
        for far, exists in ((me[axis] - 2, me[axis] > 1), (me[axis] + 2, me[axis] < sizes[axis] - 2)):
            peers += exists.astype(jnp.int32)

            @pl.when(exists)
            def _():
                pl.semaphore_signal(barrier, inc=1, device_id={axis: far}, device_id_type=MESH)
    pl.semaphore_wait(barrier, peers)

    def source(step, side, k):
        face = 0 if side == 0 else planes - 1
        at = pl.multiple_of(k * ROWS, ROWS)
        if step == 0:
            return u_ref.at[face, pl.ds(at, ROWS)]
        return bufs[step % 2].at[face, pl.ds(at + 1, ROWS)]

    def py_copy(step, side, k, device=None):
        at = pl.multiple_of(k * ROWS, ROWS)
        return pltpu.make_async_remote_copy(
            src_ref=source(step, side, k), dst_ref=halo.at[step, 1 - side, pl.ds(at, ROWS)],
            send_sem=py_send.at[step, side, k], recv_sem=py_recv.at[step, 1 - side, k],
            device_id=peer("py", side) if device is None else device, device_id_type=MESH)

    def via_copy(step, q, k, towards=1):
        return pltpu.make_async_remote_copy(
            src_ref=source(step, q, k), dst_ref=transit.at[step, k],
            send_sem=py_send.at[step, q, k], recv_sem=via_recv.at[step, k],
            device_id={"py": me["py"] + towards * (2 if q else -2)}, device_id_type=MESH)

    def on_copy(step, q, k):
        at = pl.multiple_of(k * ROWS, ROWS)
        return pltpu.make_async_remote_copy(
            src_ref=transit.at[step, k], dst_ref=halo.at[step, 1 - q, pl.ds(at, ROWS)],
            send_sem=via_send.at[step, k], recv_sem=py_recv.at[step, 1 - q, k],
            device_id=peer("py", 1 - q), device_id_type=MESH)

    def px_copy(step, side, device=None):
        edge = 0 if side == 0 else rows - 1
        src = u_ref.at[:, edge] if step == 0 else bufs[step % 2].at[:, edge + 1]
        return pltpu.make_async_remote_copy(
            src_ref=src, dst_ref=bufs[step % 2].at[:, rows + 1 if side == 0 else 0],
            send_sem=px_send.at[step, side], recv_sem=px_recv.at[step, 1 - side],
            device_id=peer("px", side) if device is None else device, device_id_type=MESH)

    def pz_copy(step, side, k, device=None):
        return pltpu.make_async_remote_copy(
            src_ref=pz_out.at[step, side, k], dst_ref=pz_in.at[step, 1 - side, k],
            send_sem=pz_send.at[step, side, k], recv_sem=pz_recv.at[step, 1 - side, k],
            device_id=peer("pz", side) if device is None else device, device_id_type=MESH)

    def pz_via_copy(step, q, k, towards=1):
        return pltpu.make_async_remote_copy(
            src_ref=pz_out.at[step, q, k], dst_ref=pz_transit.at[step, k],
            send_sem=pz_send.at[step, q, k], recv_sem=pz_via_recv.at[step, k],
            device_id={"pz": me["pz"] + towards * (2 if q else -2)}, device_id_type=MESH)

    def pz_on_copy(step, q, k):
        return pltpu.make_async_remote_copy(
            src_ref=pz_transit.at[step, k], dst_ref=pz_in.at[step, 1 - q, k],
            send_sem=pz_via_send.at[step, k], recv_sem=pz_recv.at[step, 1 - q, k],
            device_id=peer("pz", 1 - q), device_id_type=MESH)

    pz_sender = (me["pz"] == 2, me["pz"] == 1)
    pz_helper = (me["pz"] == 0, me["pz"] == 3)

    def px_start(step, side):
        @pl.when(there("px", side))
        def _():
            px_copy(step, side).start()

    def px_arrived(step, side):
        @pl.when(there("px", side))
        def _():
            px_copy(step, 1 - side, peer("px", side)).wait_recv()

    def px_sent(step, side):
        @pl.when(there("px", side))
        def _():
            px_copy(step, side).wait_send()

    def pz_start(step, k):
        for side in (0, 1):
            via = jnp.logical_and(pz_sender[side], half(k))

            @pl.when(jnp.logical_and(there("pz", side), jnp.logical_not(via)))
            def _():
                pz_copy(step, side, k).start()

            @pl.when(via)
            def _():
                pz_via_copy(step, side, k).start()

    def pz_pass(step, k):
        for q in (0, 1):
            @pl.when(jnp.logical_and(pz_helper[q], half(k)))
            def _():
                pz_via_copy(step, q, k, -1).wait_recv()
                pz_on_copy(step, q, k).start()

    def goes_via(q, k):
        return jnp.logical_and(jnp.logical_and(parity[q], there("py", q)), share(mine[q], k))

    def held(q, k):
        return jnp.logical_and(parity[q], share(others[q], k))

    def send_early(step, k):
        for q in (0, 1):
            @pl.when(goes_via(q, k))
            def _():
                via_copy(step, q, k).start()

    def send(step, k):
        for q in (0, 1):
            @pl.when(jnp.logical_and(there("py", q), jnp.logical_not(goes_via(q, k))))
            def _():
                py_copy(step, q, k).start()

            @pl.when(held(q, k))
            def _():
                via_copy(step, q, k, -1).wait_recv()
                on_copy(step, q, k).start()

    def sent(step, k):
        for q in (0, 1):
            @pl.when(there("py", q))
            def _():
                py_copy(step, q, k).wait_send()

            @pl.when(there("pz", q))
            def _():
                pz_copy(step, q, k).wait_send()

            @pl.when(jnp.logical_and(pz_helper[q], half(k)))
            def _():
                pz_on_copy(step, q, k).wait_send()

            @pl.when(held(q, k))
            def _():
                on_copy(step, q, k).wait_send()

    loop(chunks, lambda k: send_early(0, k))
    loop(EARLY, lambda k: send(0, k))
    for side in (0, 1):
        px_start(0, side)

    for side in (0, 1):
        @pl.when(jnp.logical_not(there("px", side)))
        def _():
            for slot in bufs:
                for p in range(planes):
                    slot[p, 0 if side == 0 else rows + 1] = jnp.zeros(slot.shape[2:], slot.dtype)

        @pl.when(jnp.logical_not(there("pz", side)))
        def _():
            for step in range(STEPS):
                for k in range(chunks):
                    pz_in[step, side, k] = jnp.zeros(pz_in.shape[3:], pz_in.dtype)

    loads[0].wait()

    def pack(k):
        for i in range(ROWS):
            for p in range(planes):
                pz_out[0, 0, k, p * ROWS + i:p * ROWS + i + 1] = buf0[p, k * ROWS + i + 1, 0:1]
                pz_out[0, 1, k, p * ROWS + i:p * ROWS + i + 1] = buf0[p, k * ROWS + i + 1, cols - 1:cols]
        pz_start(0, k)
    loop(chunks, pack)
    loop(AHEAD, lambda k: pz_pass(0, k))
    loop(AHEAD, lambda k: send(0, k), EARLY)
    loads[1].wait()

    inside = [there("py", side) for side in (0, 1)]

    for step in range(STEPS):
        now, later = bufs[step % 2], bufs[(step + 1) % 2]

        final = step == STEPS - 1

        def beyond(side, r):
            return jnp.where(inside[side], halo[step, side, r], 0.0)

        def outside(side, r):
            return jnp.zeros(halo.shape[3:], halo.dtype) if final else beyond(side, r)

        def complete(k):
            def row(i):
                r = k * ROWS + i
                for side, p in enumerate((0, planes - 1)):
                    later[p, r + 1] += 0.1 * beyond(side, r)
            loop(ROWS, row)

        def update(k, which):
            def row(i):
                r = k * ROWS + i
                for p in which:
                    mid = now[p, r + 1]
                    lower = outside(0, r) if p == 0 else now[p - 1, r + 1]
                    upper = outside(1, r) if p == planes - 1 else now[p + 1, r + 1]
                    left = jnp.concatenate([pz_in[step, 0, k, pl.ds(p * ROWS + i, 1)], mid[:-1]], axis=0)
                    right = jnp.concatenate([mid[1:], pz_in[step, 1, k, pl.ds(p * ROWS + i, 1)]], axis=0)
                    spread = lower + upper + now[p, r] + now[p, r + 2] + left + right - 6.0 * mid
                    new = mid + 0.1 * spread + 0.2 * mid * (1.0 - mid * inv[p, r])
                    later[p, r + 1] = new
                    if step < STEPS - 1:
                        pz_out[step + 1, 0, k, pl.ds(p * ROWS + i, 1)] = new[0:1]
                        pz_out[step + 1, 1, k, pl.ds(p * ROWS + i, 1)] = new[cols - 1:cols]
            loop(ROWS, row)

        def chunk(k):
            for side in (0, 1):
                @pl.when(there("pz", side))
                def _():
                    pz_copy(step, 1 - side, k, peer("pz", side)).wait_recv()
            if step >= 1:
                sent(step - 1, k)
            update(k, range(planes) if final else range(1, planes - 1))
            for side in (0, 1):
                @pl.when(there("py", side))
                def _():
                    py_copy(step, 1 - side, k, peer("py", side)).wait_recv()
            if final:
                complete(k)
            else:
                update(k, (0, planes - 1))
            if step < STEPS - 1:
                send_early(step + 1, k)
                pz_start(step + 1, k)

        def first(k):
            pz_pass(step, k + AHEAD)
            send(step, k + AHEAD)
            chunk(k)

        def second(k):
            chunk(k)
            if step < STEPS - 1:
                pz_pass(step + 1, k - (chunks - AHEAD))
                send(step + 1, k - (chunks - AHEAD))

        px_arrived(step, 0)
        loop(chunks - AHEAD, first)
        if step < STEPS - 1:
            px_start(step + 1, 0)
        px_arrived(step, 1)
        for side in (0, 1):
            px_sent(step, side)
        loop(chunks, second, chunks - AHEAD)
        if step < STEPS - 1:
            px_start(step + 1, 1)

    loop(chunks, lambda k: sent(STEPS - 1, k))


def drain(held_ref, out_ref, sem):
    rows = out_ref.shape[1]
    copies = [
        pltpu.make_async_copy(held_ref.at[p, pl.ds(1, rows)], out_ref.at[p], sem.at[p])
        for p in range(out_ref.shape[0])
    ]
    for copy in copies:
        copy.start()
    for copy in copies:
        copy.wait()


def local(sizes, u, inv):
    planes, rows, cols, levels = u.shape
    chunks = rows // ROWS
    dma = pltpu.SemaphoreType.DMA
    held, _ = pl.pallas_call(
        functools.partial(kernel, sizes),
        out_shape=(pltpu.VMEM((planes, rows + 2, cols, levels), u.dtype),
                   jax.ShapeDtypeStruct((STEPS, chunks, ROWS, cols, levels), u.dtype)),
        in_specs=[pl.BlockSpec(memory_space=pl.ANY)] * 2,
        out_specs=(pl.BlockSpec(memory_space=pltpu.VMEM), pl.BlockSpec(memory_space=pl.ANY)),
        scratch_shapes=[
            pltpu.VMEM((planes, rows + 2, cols, levels), u.dtype),
            pltpu.VMEM(u.shape, u.dtype),
            pltpu.VMEM((STEPS, 2, rows, cols, levels), u.dtype),
            pltpu.VMEM((STEPS, 2, chunks, planes * ROWS, levels), u.dtype),
            pltpu.VMEM((STEPS, 2, chunks, planes * ROWS, levels), u.dtype),
            dma((2,)),
            dma((STEPS, 2, chunks)),
            dma((STEPS, 2, chunks)),
            dma((STEPS, 2)),
            dma((STEPS, 2)),
            dma((STEPS, 2, chunks)),
            dma((STEPS, 2, chunks)),
            dma((STEPS, chunks)),
            dma((STEPS, chunks)),
            pltpu.VMEM((STEPS, chunks, planes * ROWS, levels), u.dtype),
            dma((STEPS, chunks)),
            dma((STEPS, chunks)),
        ],
        compiler_params=pltpu.CompilerParams(
            collective_id=0, has_side_effects=True, vmem_limit_bytes=48 * 2**20),
    )(u, inv)
    return pl.pallas_call(
        drain,
        out_shape=jax.ShapeDtypeStruct(u.shape, u.dtype),
        in_specs=[pl.BlockSpec(memory_space=pltpu.VMEM)],
        out_specs=pl.BlockSpec(memory_space=pl.ANY),
        scratch_shapes=[dma((planes,))],
        compiler_params=pltpu.CompilerParams(vmem_limit_bytes=2**20),
    )(held)


def solution(mesh):
    spec = P("py", "px", "pz", None)
    sizes = {axis: mesh.shape[axis] for axis in ("py", "px", "pz")}
    return jax.shard_map(functools.partial(local, sizes), mesh=mesh, in_specs=(spec, spec),
                         out_specs=spec, check_vma=False)
```

```python
import functools

import jax
import jax.numpy as jnp
from jax import lax
from jax.experimental import pallas as pl
from jax.experimental.pallas import tpu as pltpu
from jax.sharding import PartitionSpec as P

STEPS = 3
ROWS = 16
AHEAD = 2
EARLY = 1
MESH = pl.DeviceIdType.MESH


def share(n, k):
    return k % 4 >= 4 - n


def opens(k):
    return k % 2 == 0


def half(k):
    return k % 4 == 0


def kernel(sizes, u_ref, inv_ref, out_ref, transit, buf0, inv, halo, pz_in, pz_out,
           load_sem, py_send, py_recv, px_send, px_recv, pz_send, pz_recv,
           via_send, via_recv, pz_transit, pz_via_send, pz_via_recv):
    planes, rows, cols, _ = u_ref.shape
    chunks = rows // ROWS
    bufs = (buf0, out_ref)
    me = {axis: lax.axis_index(axis) for axis in sizes}
    last = sizes["py"] - 1
    parity = [me["py"] % 2 == 0, me["py"] % 2 == 1]
    mine = ((last + 1 - me["py"]) // 2, (me["py"] + 1) // 2)
    others = ((last - 1 - me["py"]) // 2, (me["py"] - 1) // 2)

    def there(axis, side):
        return me[axis] > 0 if side == 0 else me[axis] < sizes[axis] - 1

    def peer(axis, side):
        return {axis: me[axis] + (1 if side else -1)}

    def loop(count, body, start=0):
        def step(k, carry):
            body(k)
            return carry
        lax.fori_loop(start, count, step, 0)

    loads = [
        pltpu.make_async_copy(u_ref, buf0.at[:, pl.ds(1, rows)], load_sem.at[0]),
        pltpu.make_async_copy(inv_ref, inv, load_sem.at[1]),
    ]

    barrier = pltpu.get_barrier_semaphore()
    peers = jnp.int32(0)
    for axis in sizes:
        for side in (0, 1):
            peers += there(axis, side).astype(jnp.int32)

            @pl.when(there(axis, side))
            def _():
                pl.semaphore_signal(barrier, inc=1, device_id=peer(axis, side), device_id_type=MESH)
    for axis in ("py", "pz"):
        for far, exists in ((me[axis] - 2, me[axis] > 1), (me[axis] + 2, me[axis] < sizes[axis] - 2)):
            peers += exists.astype(jnp.int32)

            @pl.when(exists)
            def _():
                pl.semaphore_signal(barrier, inc=1, device_id={axis: far}, device_id_type=MESH)
    pl.semaphore_wait(barrier, peers)

    def source(step, side, k):
        face = 0 if side == 0 else planes - 1
        at = pl.multiple_of(k * ROWS, ROWS)
        if step == 0:
            return u_ref.at[face, pl.ds(at, ROWS)]
        return bufs[step % 2].at[face, pl.ds(at + 1, ROWS)]

    def py_copy(step, side, k, device=None):
        at = pl.multiple_of(k * ROWS, ROWS)
        return pltpu.make_async_remote_copy(
            src_ref=source(step, side, k), dst_ref=halo.at[step, 1 - side, pl.ds(at, ROWS)],
            send_sem=py_send.at[step, side, k], recv_sem=py_recv.at[step, 1 - side, k],
            device_id=peer("py", side) if device is None else device, device_id_type=MESH)

    def via_copy(step, q, k, towards=1):
        return pltpu.make_async_remote_copy(
            src_ref=source(step, q, k), dst_ref=transit.at[step, k],
            send_sem=py_send.at[step, q, k], recv_sem=via_recv.at[step, k],
            device_id={"py": me["py"] + towards * (2 if q else -2)}, device_id_type=MESH)

    def on_copy(step, q, k):
        at = pl.multiple_of(k * ROWS, ROWS)
        return pltpu.make_async_remote_copy(
            src_ref=transit.at[step, k], dst_ref=halo.at[step, 1 - q, pl.ds(at, ROWS)],
            send_sem=via_send.at[step, k], recv_sem=py_recv.at[step, 1 - q, k],
            device_id=peer("py", 1 - q), device_id_type=MESH)

    def px_copy(step, side, device=None):
        edge = 0 if side == 0 else rows - 1
        src = u_ref.at[:, edge] if step == 0 else bufs[step % 2].at[:, edge + 1]
        return pltpu.make_async_remote_copy(
            src_ref=src, dst_ref=bufs[step % 2].at[:, rows + 1 if side == 0 else 0],
            send_sem=px_send.at[step, side], recv_sem=px_recv.at[step, 1 - side],
            device_id=peer("px", side) if device is None else device, device_id_type=MESH)

    def pz_copy(step, side, k, device=None):
        return pltpu.make_async_remote_copy(
            src_ref=pz_out.at[step, side, pl.ds(k, 2)], dst_ref=pz_in.at[step, 1 - side, pl.ds(k, 2)],
            send_sem=pz_send.at[step, side, k], recv_sem=pz_recv.at[step, 1 - side, k],
            device_id=peer("pz", side) if device is None else device, device_id_type=MESH)

    def pz_via_copy(step, q, k, towards=1):
        return pltpu.make_async_remote_copy(
            src_ref=pz_out.at[step, q, pl.ds(k, 2)], dst_ref=pz_transit.at[step, pl.ds(k, 2)],
            send_sem=pz_send.at[step, q, k], recv_sem=pz_via_recv.at[step, k],
            device_id={"pz": me["pz"] + towards * (2 if q else -2)}, device_id_type=MESH)

    def pz_on_copy(step, q, k):
        return pltpu.make_async_remote_copy(
            src_ref=pz_transit.at[step, pl.ds(k, 2)], dst_ref=pz_in.at[step, 1 - q, pl.ds(k, 2)],
            send_sem=pz_via_send.at[step, k], recv_sem=pz_recv.at[step, 1 - q, k],
            device_id=peer("pz", 1 - q), device_id_type=MESH)

    pz_sender = (me["pz"] == 2, me["pz"] == 1)
    pz_helper = (me["pz"] == 0, me["pz"] == 3)

    def px_start(step, side):
        @pl.when(there("px", side))
        def _():
            px_copy(step, side).start()

    def px_arrived(step, side):
        @pl.when(there("px", side))
        def _():
            px_copy(step, 1 - side, peer("px", side)).wait_recv()

    def px_sent(step, side):
        @pl.when(there("px", side))
        def _():
            px_copy(step, side).wait_send()

    def pz_start(step, k):
        for side in (0, 1):
            via = jnp.logical_and(pz_sender[side], half(k))

            @pl.when(jnp.logical_and(there("pz", side), jnp.logical_not(via)))
            def _():
                pz_copy(step, side, k).start()

            @pl.when(via)
            def _():
                pz_via_copy(step, side, k).start()

    def pz_pass(step, k):
        for q in (0, 1):
            @pl.when(jnp.logical_and(pz_helper[q], half(k)))
            def _():
                pz_via_copy(step, q, k, -1).wait_recv()
                pz_on_copy(step, q, k).start()

    def goes_via(q, k):
        return jnp.logical_and(jnp.logical_and(parity[q], there("py", q)), share(mine[q], k))

    def held(q, k):
        return jnp.logical_and(parity[q], share(others[q], k))

    def send_early(step, k):
        for q in (0, 1):
            @pl.when(goes_via(q, k))
            def _():
                via_copy(step, q, k).start()

    def send(step, k):
        for q in (0, 1):
            @pl.when(jnp.logical_and(there("py", q), jnp.logical_not(goes_via(q, k))))
            def _():
                py_copy(step, q, k).start()

            @pl.when(held(q, k))
            def _():
                via_copy(step, q, k, -1).wait_recv()
                on_copy(step, q, k).start()

    def sent(step, k):
        for q in (0, 1):
            @pl.when(there("py", q))
            def _():
                py_copy(step, q, k).wait_send()

            @pl.when(jnp.logical_and(there("pz", q), opens(k)))
            def _():
                pz_copy(step, q, k).wait_send()

            @pl.when(jnp.logical_and(pz_helper[q], half(k)))
            def _():
                pz_on_copy(step, q, k).wait_send()

            @pl.when(held(q, k))
            def _():
                on_copy(step, q, k).wait_send()

    loop(chunks, lambda k: send_early(0, k))
    loop(EARLY, lambda k: send(0, k))
    loads[0].start()
    for side in (0, 1):
        px_start(0, side)
    loads[1].start()

    for side in (0, 1):
        @pl.when(jnp.logical_not(there("px", side)))
        def _():
            for slot in bufs:
                for p in range(planes):
                    slot[p, 0 if side == 0 else rows + 1] = jnp.zeros(slot.shape[2:], slot.dtype)

        @pl.when(jnp.logical_not(there("pz", side)))
        def _():
            for step in range(STEPS):
                for k in range(chunks):
                    pz_in[step, side, k] = jnp.zeros(pz_in.shape[3:], pz_in.dtype)

    loads[0].wait()

    def pack(k):
        for i in range(ROWS):
            for p in range(planes):
                pz_out[0, 0, k, p * ROWS + i:p * ROWS + i + 1] = buf0[p, k * ROWS + i + 1, 0:1]
                pz_out[0, 1, k, p * ROWS + i:p * ROWS + i + 1] = buf0[p, k * ROWS + i + 1, cols - 1:cols]

        @pl.when(jnp.logical_not(opens(k)))
        def _():
            pz_start(0, k - 1)
    loop(chunks, pack)
    loop(AHEAD, lambda k: pz_pass(0, k))
    loop(AHEAD, lambda k: send(0, k), EARLY)
    loads[1].wait()

    inside = [there("py", side) for side in (0, 1)]

    for step in range(STEPS):
        now, later = bufs[step % 2], bufs[(step + 1) % 2]

        final = step == STEPS - 1

        def beyond(side, r):
            return jnp.where(inside[side], halo[step, side, r], 0.0)

        def outside(side, r):
            return jnp.zeros(halo.shape[3:], halo.dtype) if final else beyond(side, r)

        def complete(k):
            def row(i):
                r = k * ROWS + i
                for side, p in enumerate((0, planes - 1)):
                    later[p, r + 1] += 0.1 * beyond(side, r)
            loop(ROWS, row)

        def update(k, which):
            def row(i):
                r = k * ROWS + i
                for p in which:
                    mid = now[p, r + 1]
                    lower = outside(0, r) if p == 0 else now[p - 1, r + 1]
                    upper = outside(1, r) if p == planes - 1 else now[p + 1, r + 1]
                    left = jnp.concatenate([pz_in[step, 0, k, pl.ds(p * ROWS + i, 1)], mid[:-1]], axis=0)
                    right = jnp.concatenate([mid[1:], pz_in[step, 1, k, pl.ds(p * ROWS + i, 1)]], axis=0)
                    spread = lower + upper + now[p, r] + now[p, r + 2] + left + right - 6.0 * mid
                    new = mid + 0.1 * spread + 0.2 * mid * (1.0 - mid * inv[p, r])
                    later[p, r + 1] = new
                    if step < STEPS - 1:
                        pz_out[step + 1, 0, k, pl.ds(p * ROWS + i, 1)] = new[0:1]
                        pz_out[step + 1, 1, k, pl.ds(p * ROWS + i, 1)] = new[cols - 1:cols]
            loop(ROWS, row)

        def chunk(k):
            for side in (0, 1):
                @pl.when(jnp.logical_and(there("pz", side), opens(k)))
                def _():
                    pz_copy(step, 1 - side, k, peer("pz", side)).wait_recv()
            if step >= 1:
                sent(step - 1, k)
            update(k, range(planes) if final else range(1, planes - 1))
            for side in (0, 1):
                @pl.when(there("py", side))
                def _():
                    py_copy(step, 1 - side, k, peer("py", side)).wait_recv()
            if final:
                complete(k)
            else:
                update(k, (0, planes - 1))
            if step < STEPS - 1:
                send_early(step + 1, k)

                @pl.when(jnp.logical_not(opens(k)))
                def _():
                    pz_start(step + 1, k - 1)

        def first(k):
            pz_pass(step, k + AHEAD)
            send(step, k + AHEAD)
            chunk(k)

        def second(k):
            chunk(k)
            if step < STEPS - 1:
                pz_pass(step + 1, k - (chunks - AHEAD))
                send(step + 1, k - (chunks - AHEAD))

        px_arrived(step, 0)
        loop(chunks - AHEAD, first)
        if step < STEPS - 1:
            px_start(step + 1, 0)
        px_arrived(step, 1)
        for side in (0, 1):
            px_sent(step, side)
        loop(chunks, second, chunks - AHEAD)
        if step < STEPS - 1:
            px_start(step + 1, 1)

    loop(chunks, lambda k: sent(STEPS - 1, k))


def drain(held_ref, out_ref, sem):
    rows = out_ref.shape[1]
    copies = [
        pltpu.make_async_copy(held_ref.at[p, pl.ds(1, rows)], out_ref.at[p], sem.at[p])
        for p in range(out_ref.shape[0])
    ]
    for copy in copies:
        copy.start()
    for copy in copies:
        copy.wait()


def local(sizes, u, inv):
    planes, rows, cols, levels = u.shape
    chunks = rows // ROWS
    dma = pltpu.SemaphoreType.DMA
    held, _ = pl.pallas_call(
        functools.partial(kernel, sizes),
        out_shape=(pltpu.VMEM((planes, rows + 2, cols, levels), u.dtype),
                   jax.ShapeDtypeStruct((STEPS, chunks, ROWS, cols, levels), u.dtype)),
        in_specs=[pl.BlockSpec(memory_space=pl.ANY)] * 2,
        out_specs=(pl.BlockSpec(memory_space=pltpu.VMEM), pl.BlockSpec(memory_space=pl.ANY)),
        scratch_shapes=[
            pltpu.VMEM((planes, rows + 2, cols, levels), u.dtype),
            pltpu.VMEM(u.shape, u.dtype),
            pltpu.VMEM((STEPS, 2, rows, cols, levels), u.dtype),
            pltpu.VMEM((STEPS, 2, chunks, planes * ROWS, levels), u.dtype),
            pltpu.VMEM((STEPS, 2, chunks, planes * ROWS, levels), u.dtype),
            dma((2,)),
            dma((STEPS, 2, chunks)),
            dma((STEPS, 2, chunks)),
            dma((STEPS, 2)),
            dma((STEPS, 2)),
            dma((STEPS, 2, chunks)),
            dma((STEPS, 2, chunks)),
            dma((STEPS, chunks)),
            dma((STEPS, chunks)),
            pltpu.VMEM((STEPS, chunks, planes * ROWS, levels), u.dtype),
            dma((STEPS, chunks)),
            dma((STEPS, chunks)),
        ],
        compiler_params=pltpu.CompilerParams(
            collective_id=0, has_side_effects=True, vmem_limit_bytes=48 * 2**20),
    )(u, inv)
    return pl.pallas_call(
        drain,
        out_shape=jax.ShapeDtypeStruct(u.shape, u.dtype),
        in_specs=[pl.BlockSpec(memory_space=pltpu.VMEM)],
        out_specs=pl.BlockSpec(memory_space=pl.ANY),
        scratch_shapes=[dma((planes,))],
        compiler_params=pltpu.CompilerParams(vmem_limit_bytes=2**20),
    )(held)


def solution(mesh):
    spec = P("py", "px", "pz", None)
    sizes = {axis: mesh.shape[axis] for axis in ("py", "px", "pz")}
    return jax.shard_map(functools.partial(local, sizes), mesh=mesh, in_specs=(spec, spec),
                         out_specs=spec, check_vma=False)
```

```python
import functools

import jax
import jax.numpy as jnp
from jax import lax
from jax.experimental import pallas as pl
from jax.experimental.pallas import tpu as pltpu
from jax.sharding import PartitionSpec as P

STEPS = 3
ROWS = 16
AHEAD = 2
EARLY = 1
MESH = pl.DeviceIdType.MESH


def share(n, k):
    return k % 4 >= 4 - n


def opens(k):
    return k % 2 == 0


def half(k):
    return k % 4 == 0


def kernel(sizes, u_ref, inv_ref, out_ref, transit, buf0, inv, halo, pz_in, pz_out,
           load_sem, py_send, py_recv, px_send, px_recv, pz_send, pz_recv,
           via_send, via_recv, pz_transit, pz_via_send, pz_via_recv):
    planes, rows, cols, _ = u_ref.shape
    chunks = rows // ROWS
    bufs = (buf0, out_ref)
    me = {axis: lax.axis_index(axis) for axis in sizes}
    last = sizes["py"] - 1
    parity = [me["py"] % 2 == 0, me["py"] % 2 == 1]
    mine = ((last + 1 - me["py"]) // 2, (me["py"] + 1) // 2)
    others = ((last - 1 - me["py"]) // 2, (me["py"] - 1) // 2)

    def there(axis, side):
        return me[axis] > 0 if side == 0 else me[axis] < sizes[axis] - 1

    def peer(axis, side):
        return {axis: me[axis] + (1 if side else -1)}

    def loop(count, body, start=0):
        def step(k, carry):
            body(k)
            return carry
        lax.fori_loop(start, count, step, 0)

    loads = [
        pltpu.make_async_copy(u_ref, buf0.at[:, pl.ds(1, rows)], load_sem.at[0]),
        pltpu.make_async_copy(inv_ref, inv, load_sem.at[1]),
    ]

    barrier = pltpu.get_barrier_semaphore()
    peers = jnp.int32(0)
    for axis in sizes:
        for side in (0, 1):
            peers += there(axis, side).astype(jnp.int32)

            @pl.when(there(axis, side))
            def _():
                pl.semaphore_signal(barrier, inc=1, device_id=peer(axis, side), device_id_type=MESH)
    for axis in ("py", "pz"):
        for far, exists in ((me[axis] - 2, me[axis] > 1), (me[axis] + 2, me[axis] < sizes[axis] - 2)):
            peers += exists.astype(jnp.int32)

            @pl.when(exists)
            def _():
                pl.semaphore_signal(barrier, inc=1, device_id={axis: far}, device_id_type=MESH)
    pl.semaphore_wait(barrier, peers)

    def source(step, side, k):
        face = 0 if side == 0 else planes - 1
        at = pl.multiple_of(k * ROWS, ROWS)
        if step == 0:
            return u_ref.at[face, pl.ds(at, ROWS)]
        return bufs[step % 2].at[face, pl.ds(at + 1, ROWS)]

    def py_copy(step, side, k, device=None):
        at = pl.multiple_of(k * ROWS, ROWS)
        return pltpu.make_async_remote_copy(
            src_ref=source(step, side, k), dst_ref=halo.at[step, 1 - side, pl.ds(at, ROWS)],
            send_sem=py_send.at[step, side, k], recv_sem=py_recv.at[step, 1 - side, k],
            device_id=peer("py", side) if device is None else device, device_id_type=MESH)

    def via_copy(step, q, k, towards=1):
        return pltpu.make_async_remote_copy(
            src_ref=source(step, q, k), dst_ref=transit.at[step, k],
            send_sem=py_send.at[step, q, k], recv_sem=via_recv.at[step, k],
            device_id={"py": me["py"] + towards * (2 if q else -2)}, device_id_type=MESH)

    def on_copy(step, q, k):
        at = pl.multiple_of(k * ROWS, ROWS)
        return pltpu.make_async_remote_copy(
            src_ref=transit.at[step, k], dst_ref=halo.at[step, 1 - q, pl.ds(at, ROWS)],
            send_sem=via_send.at[step, k], recv_sem=py_recv.at[step, 1 - q, k],
            device_id=peer("py", 1 - q), device_id_type=MESH)

    def px_copy(step, side, device=None):
        edge = 0 if side == 0 else rows - 1
        src = u_ref.at[:, edge] if step == 0 else bufs[step % 2].at[:, edge + 1]
        return pltpu.make_async_remote_copy(
            src_ref=src, dst_ref=bufs[step % 2].at[:, rows + 1 if side == 0 else 0],
            send_sem=px_send.at[step, side], recv_sem=px_recv.at[step, 1 - side],
            device_id=peer("px", side) if device is None else device, device_id_type=MESH)

    def pz_copy(step, side, k, device=None):
        return pltpu.make_async_remote_copy(
            src_ref=pz_out.at[step, side, pl.ds(k, 2)], dst_ref=pz_in.at[step, 1 - side, pl.ds(k, 2)],
            send_sem=pz_send.at[step, side, k], recv_sem=pz_recv.at[step, 1 - side, k],
            device_id=peer("pz", side) if device is None else device, device_id_type=MESH)

    def pz_via_copy(step, q, k, towards=1):
        return pltpu.make_async_remote_copy(
            src_ref=pz_out.at[step, q, pl.ds(k, 2)], dst_ref=pz_transit.at[step, pl.ds(k, 2)],
            send_sem=pz_send.at[step, q, k], recv_sem=pz_via_recv.at[step, k],
            device_id={"pz": me["pz"] + towards * (2 if q else -2)}, device_id_type=MESH)

    def pz_on_copy(step, q, k):
        return pltpu.make_async_remote_copy(
            src_ref=pz_transit.at[step, pl.ds(k, 2)], dst_ref=pz_in.at[step, 1 - q, pl.ds(k, 2)],
            send_sem=pz_via_send.at[step, k], recv_sem=pz_recv.at[step, 1 - q, k],
            device_id=peer("pz", 1 - q), device_id_type=MESH)

    pz_sender = (me["pz"] == 2, me["pz"] == 1)
    pz_helper = (me["pz"] == 0, me["pz"] == 3)

    def px_start(step, side):
        @pl.when(there("px", side))
        def _():
            px_copy(step, side).start()

    def px_arrived(step, side):
        @pl.when(there("px", side))
        def _():
            px_copy(step, 1 - side, peer("px", side)).wait_recv()

    def px_sent(step, side):
        @pl.when(there("px", side))
        def _():
            px_copy(step, side).wait_send()

    def pz_start(step, k):
        for side in (0, 1):
            via = jnp.logical_and(pz_sender[side], half(k))

            @pl.when(jnp.logical_and(there("pz", side), jnp.logical_not(via)))
            def _():
                pz_copy(step, side, k).start()

            @pl.when(via)
            def _():
                pz_via_copy(step, side, k).start()

    def pz_pass(step, k):
        for q in (0, 1):
            @pl.when(jnp.logical_and(pz_helper[q], half(k)))
            def _():
                pz_via_copy(step, q, k, -1).wait_recv()
                pz_on_copy(step, q, k).start()

    def goes_via(q, k):
        return jnp.logical_and(jnp.logical_and(parity[q], there("py", q)), share(mine[q], k))

    def held(q, k):
        return jnp.logical_and(parity[q], share(others[q], k))

    def send_early(step, k):
        for q in (0, 1):
            @pl.when(goes_via(q, k))
            def _():
                via_copy(step, q, k).start()

    def send(step, k):
        for q in (0, 1):
            @pl.when(jnp.logical_and(parity[1 - q], there("py", q)))
            def _():
                py_copy(step, q, k).start()

        for q in (0, 1):
            @pl.when(jnp.logical_and(jnp.logical_and(parity[q], there("py", q)), jnp.logical_not(goes_via(q, k))))
            def _():
                py_copy(step, q, k).start()

            @pl.when(held(q, k))
            def _():
                via_copy(step, q, k, -1).wait_recv()
                on_copy(step, q, k).start()

    def sent(step, k):
        for q in (0, 1):
            @pl.when(there("py", q))
            def _():
                py_copy(step, q, k).wait_send()

            @pl.when(jnp.logical_and(there("pz", q), opens(k)))
            def _():
                pz_copy(step, q, k).wait_send()

            @pl.when(jnp.logical_and(pz_helper[q], half(k)))
            def _():
                pz_on_copy(step, q, k).wait_send()

            @pl.when(held(q, k))
            def _():
                on_copy(step, q, k).wait_send()

    loop(chunks, lambda k: send_early(0, k))
    loop(EARLY, lambda k: send(0, k))
    loads[0].start()
    for side in (0, 1):
        px_start(0, side)
    loads[1].start()

    for side in (0, 1):
        @pl.when(jnp.logical_not(there("px", side)))
        def _():
            for slot in bufs:
                for p in range(planes):
                    slot[p, 0 if side == 0 else rows + 1] = jnp.zeros(slot.shape[2:], slot.dtype)

        @pl.when(jnp.logical_not(there("pz", side)))
        def _():
            for step in range(STEPS):
                for k in range(chunks):
                    pz_in[step, side, k] = jnp.zeros(pz_in.shape[3:], pz_in.dtype)

    loads[0].wait()

    def pack(k):
        for i in range(ROWS):
            for p in range(planes):
                pz_out[0, 0, k, p * ROWS + i:p * ROWS + i + 1] = buf0[p, k * ROWS + i + 1, 0:1]
                pz_out[0, 1, k, p * ROWS + i:p * ROWS + i + 1] = buf0[p, k * ROWS + i + 1, cols - 1:cols]

        @pl.when(jnp.logical_not(opens(k)))
        def _():
            pz_start(0, k - 1)
    loop(chunks, pack)
    loop(AHEAD, lambda k: pz_pass(0, k))
    loop(AHEAD, lambda k: send(0, k), EARLY)
    loads[1].wait()

    inside = [there("py", side) for side in (0, 1)]

    for step in range(STEPS):
        now, later = bufs[step % 2], bufs[(step + 1) % 2]

        final = step == STEPS - 1

        def beyond(side, r):
            return jnp.where(inside[side], halo[step, side, r], 0.0)

        def outside(side, r):
            return jnp.zeros(halo.shape[3:], halo.dtype) if final else beyond(side, r)

        def complete(k):
            def row(i):
                r = k * ROWS + i
                for side, p in enumerate((0, planes - 1)):
                    later[p, r + 1] += 0.1 * beyond(side, r)
            loop(ROWS, row)

        def update(k, which):
            def row(i):
                r = k * ROWS + i
                for p in which:
                    mid = now[p, r + 1]
                    lower = outside(0, r) if p == 0 else now[p - 1, r + 1]
                    upper = outside(1, r) if p == planes - 1 else now[p + 1, r + 1]
                    left = jnp.concatenate([pz_in[step, 0, k, pl.ds(p * ROWS + i, 1)], mid[:-1]], axis=0)
                    right = jnp.concatenate([mid[1:], pz_in[step, 1, k, pl.ds(p * ROWS + i, 1)]], axis=0)
                    spread = lower + upper + now[p, r] + now[p, r + 2] + left + right - 6.0 * mid
                    new = mid + 0.1 * spread + 0.2 * mid * (1.0 - mid * inv[p, r])
                    later[p, r + 1] = new
                    if step < STEPS - 1:
                        pz_out[step + 1, 0, k, pl.ds(p * ROWS + i, 1)] = new[0:1]
                        pz_out[step + 1, 1, k, pl.ds(p * ROWS + i, 1)] = new[cols - 1:cols]
            loop(ROWS, row)

        def chunk(k):
            for side in (0, 1):
                @pl.when(jnp.logical_and(there("pz", side), opens(k)))
                def _():
                    pz_copy(step, 1 - side, k, peer("pz", side)).wait_recv()
            if step >= 1:
                sent(step - 1, k)
            update(k, range(planes) if final else range(1, planes - 1))
            for side in (0, 1):
                @pl.when(there("py", side))
                def _():
                    py_copy(step, 1 - side, k, peer("py", side)).wait_recv()
            if final:
                complete(k)
            else:
                update(k, (0, planes - 1))
            if step < STEPS - 1:
                send_early(step + 1, k)

                @pl.when(jnp.logical_not(opens(k)))
                def _():
                    pz_start(step + 1, k - 1)

        def first(k):
            pz_pass(step, k + AHEAD)
            send(step, k + AHEAD)
            chunk(k)

        def second(k):
            chunk(k)
            if step < STEPS - 1:
                pz_pass(step + 1, k - (chunks - AHEAD))
                send(step + 1, k - (chunks - AHEAD))

        px_arrived(step, 0)
        loop(chunks - AHEAD, first)
        if step < STEPS - 1:
            px_start(step + 1, 0)
        px_arrived(step, 1)
        for side in (0, 1):
            px_sent(step, side)
        loop(chunks, second, chunks - AHEAD)
        if step < STEPS - 1:
            px_start(step + 1, 1)

    loop(chunks, lambda k: sent(STEPS - 1, k))


def drain(held_ref, out_ref, sem):
    rows = out_ref.shape[1]
    copies = [
        pltpu.make_async_copy(held_ref.at[p, pl.ds(1, rows)], out_ref.at[p], sem.at[p])
        for p in range(out_ref.shape[0])
    ]
    for copy in copies:
        copy.start()
    for copy in copies:
        copy.wait()


def local(sizes, u, inv):
    planes, rows, cols, levels = u.shape
    chunks = rows // ROWS
    dma = pltpu.SemaphoreType.DMA
    held, _ = pl.pallas_call(
        functools.partial(kernel, sizes),
        out_shape=(pltpu.VMEM((planes, rows + 2, cols, levels), u.dtype),
                   jax.ShapeDtypeStruct((STEPS, chunks, ROWS, cols, levels), u.dtype)),
        in_specs=[pl.BlockSpec(memory_space=pl.ANY)] * 2,
        out_specs=(pl.BlockSpec(memory_space=pltpu.VMEM), pl.BlockSpec(memory_space=pl.ANY)),
        scratch_shapes=[
            pltpu.VMEM((planes, rows + 2, cols, levels), u.dtype),
            pltpu.VMEM(u.shape, u.dtype),
            pltpu.VMEM((STEPS, 2, rows, cols, levels), u.dtype),
            pltpu.VMEM((STEPS, 2, chunks, planes * ROWS, levels), u.dtype),
            pltpu.VMEM((STEPS, 2, chunks, planes * ROWS, levels), u.dtype),
            dma((2,)),
            dma((STEPS, 2, chunks)),
            dma((STEPS, 2, chunks)),
            dma((STEPS, 2)),
            dma((STEPS, 2)),
            dma((STEPS, 2, chunks)),
            dma((STEPS, 2, chunks)),
            dma((STEPS, chunks)),
            dma((STEPS, chunks)),
            pltpu.VMEM((STEPS, chunks, planes * ROWS, levels), u.dtype),
            dma((STEPS, chunks)),
            dma((STEPS, chunks)),
        ],
        compiler_params=pltpu.CompilerParams(
            collective_id=0, has_side_effects=True, vmem_limit_bytes=48 * 2**20),
    )(u, inv)
    return pl.pallas_call(
        drain,
        out_shape=jax.ShapeDtypeStruct(u.shape, u.dtype),
        in_specs=[pl.BlockSpec(memory_space=pltpu.VMEM)],
        out_specs=pl.BlockSpec(memory_space=pl.ANY),
        scratch_shapes=[dma((planes,))],
        compiler_params=pltpu.CompilerParams(vmem_limit_bytes=2**20),
    )(held)


def solution(mesh):
    spec = P("py", "px", "pz", None)
    sizes = {axis: mesh.shape[axis] for axis in ("py", "px", "pz")}
    return jax.shard_map(functools.partial(local, sizes), mesh=mesh, in_specs=(spec, spec),
                         out_specs=spec, check_vma=False)
```
